32 devices in a mesh: band: 8 (over z, x), slab: 4 (over y, core).
Axes of the slice: x: 2, y: 2, z: 4, core: 2. Of those that a mesh axis runs over, the one named last changes fastest.
Arguments:
- orbitals: float32 [512, 64, 512], P('band', 'slab'), may hold values from -6 to 6
- potential: float32 [64, 512], P('slab'), may hold values from 0 to 1
- projectors: float32 [4, 2048, 128], replicated, may hold values from -0.125 to 0.125
- atom_kind: int32 [32], P('slab'), may hold values from 0 to 3
- atom_plane: int32 [32], P('slab'), may hold values from 0 to 60, as said below
- atom_coef: float32 [32, 128], P('slab'), may hold values from 0.2 to 1
- filter_cut: float32 [1], replicated, may hold values from 0.5 to 2
- filter_top: float32 [1], replicated, may hold values from 9 to 14
Outputs:
- new_orbitals: float32 [512, 32768], P(None, ('slab', 'band'))
The draws below stay inside these ranges and needn't reach their ends.
Inputs may be any that keep to these rules, and one draw needn't show every extreme that they name: `atom_plane`: block i's 4 planes lie inside the slab of planes (i // 8) * 16 to (i // 8 + 1) * 16 - 1; blocks may share planes.
All inputs are finite; a program needn't handle non-finite values.
Results may differ from the reference program's by a relative error of at most 0.0003.
Values sent between devices are 32-bit elements; how exact they have to be, the bound alone decides.
A program may use at most 128 MiB of HBM per device.

```python
import math
import jax
import jax.numpy as jnp
from jax import lax

NB = 512
FUNCS = 128
CX = 16
GY = 16
GZ = 32
BP = 4
KINDS = 4
ATOM_SLAB = 8
ORDER = 6
GX = 64
NPTS = 32768
ATOMS = 32
BPTS = 2048


def draw_atom_plane(key, part):
    atom_ids = jnp.arange(ATOMS).astype(jnp.int32)
    slab_ids = atom_ids // ATOM_SLAB
    offsets = jax.random.randint(key, (ATOMS,), 0, CX - BP + 1).astype(jnp.int32)
    return (slab_ids * CX + offsets).astype(jnp.int32)


def set_ends(array, key, least, largest):
    longest = array.shape.index(max(array.shape))
    spots = []
    for shift in (0, 1):
        where = [jax.random.randint(jax.random.fold_in(key, axis), (), 0, length) for axis, length in enumerate(array.shape)]
        where[longest] = (where[longest] + shift) % array.shape[longest]
        spots.append(tuple(where))
    return array.at[spots[0]].set(least).at[spots[1]].set(largest)


def block_levels(stream_key, extent, split, least, high):
    loudness, own = 1.0, jax.random.fold_in(stream_key, 6)
    for dim, parts in split:
        steps = jnp.exp(jax.random.uniform(jax.random.fold_in(own, dim), (parts,), jnp.float32, least / len(split), high / len(split)))
        loudness = loudness * jnp.repeat(steps, extent[dim] // parts).reshape([-1 if axis == dim else 1 for axis in range(len(extent))])
    return loudness


def bell_draw(key, shape, deviation, limit, pieces=(), held_as=jnp.bfloat16):
    entries = deviation * jax.random.normal(key, shape, jnp.float32)
    if pieces:
        entries = entries * block_levels(key, shape, pieces, -0.22, 0.18)
    return jnp.clip(entries, -limit, limit).astype(held_as)


def setup_inputs(seed: int = 0) -> dict:
    splits = jax.random.split(jax.random.key(seed), 9)
    return {
        "orbitals": bell_draw(splits[0], (NB, GX, GY * GZ), 1.0, 6.0, ((0, 8), (1, 4)), jnp.float32),
        "potential": jnp.clip(1.0 * jax.random.uniform(splits[1], (GX, GY * GZ), jnp.float32) ** block_levels(splits[1], (GX, GY * GZ), ((0, 4),), -0.2, 0.2), 0.0, 1.0),
        "projectors": bell_draw(splits[2], (KINDS, BPTS, FUNCS), BPTS ** -0.5, 0.125, (), jnp.float32),
        "atom_kind": set_ends(jax.random.randint(splits[3], (ATOMS,), 0, KINDS), jax.random.fold_in(splits[3], 1), 0, KINDS - 1).astype(jnp.int32),
        "atom_plane": draw_atom_plane(jax.random.fold_in(splits[8], 71), 0),
        "atom_coef": jnp.clip(jnp.exp(math.log(1.0) - 1.609438 * jax.random.uniform(splits[5], (ATOMS, FUNCS), jnp.float32) ** block_levels(splits[5], (ATOMS, FUNCS), ((0, 4),), -0.2, 0.2)), 0.2, 1.0),
        "filter_cut": jnp.clip(jax.random.uniform(splits[6], (1,), jnp.float32, 0.5, 2.0), 0.5, 2.0),
        "filter_top": jnp.clip(jax.random.uniform(splits[7], (1,), jnp.float32, 9.0, 14.0), 9.0, 14.0),
    }


low_edge = -1.0
near_coef = 4.0 / 3.0
far_coef = -1.0 / 12.0
self_coef = -2.5
highest = lax.Precision.HIGHEST

def shifted(source, offset):
    if offset > 0:
        zeros_part = jnp.zeros(source.shape[:-1] + (offset,), source.dtype)
        return jnp.concatenate([zeros_part, source[..., :-offset]], axis=-1)
    zeros_part = jnp.zeros(source.shape[:-1] + (-offset,), source.dtype)
    return jnp.concatenate([source[..., -offset:], zeros_part], axis=-1)

def transverse(source, width_z):
    length_last = source.shape[-1]
    z_position = jnp.arange(length_last) % width_z
    result_sum = 2.0 * self_coef * source
    for offset, weight_coef in ((1, near_coef), (-1, near_coef), (2, far_coef), (-2, far_coef)):
        result_sum = result_sum + weight_coef * shifted(source, offset * width_z)
        inside = (z_position - offset >= 0) & (z_position - offset < width_z)
        result_sum = result_sum + weight_coef * jnp.where(inside, shifted(source, offset), 0.0)
    return result_sum

def hamiltonian(source, potential, selector, atom_tables, atom_coef):
    along_x = self_coef * source
    along_x = along_x + near_coef * (jnp.roll(source, 1, axis=1) + jnp.roll(source, -1, axis=1))
    along_x = along_x + far_coef * (jnp.roll(source, 2, axis=1) + jnp.roll(source, -2, axis=1))
    laplace = along_x + transverse(source, GZ)
    atom_count = selector.shape[0]
    orbital_count = source.shape[0]
    blocks = jnp.einsum('ajx,nxp->anjp', selector, source, precision=highest)
    blocks = blocks.reshape(atom_count, orbital_count, BPTS)
    coupled = jnp.einsum('anq,aqf->anf', blocks, atom_tables, precision=highest) * atom_coef[:, None, :]
    spread_back = jnp.einsum('anf,aqf->anq', coupled, atom_tables, precision=highest)
    spread_back = spread_back.reshape(atom_count, orbital_count, BP, GY * GZ)
    nonlocal_part = jnp.einsum('ajx,anjp->nxp', selector, spread_back, precision=highest)
    return -0.5 * laplace + potential[None] * source + nonlocal_part

def chebyshev(start, hamiltonian_fn, cut_value, top_value):
    half_width = (top_value - cut_value) / 2.0
    centre = (top_value + cut_value) / 2.0
    sigma_now = half_width / (low_edge - centre)
    tau_value = 2.0 / sigma_now
    previous = start
    current = (hamiltonian_fn(previous) - centre * previous) * (sigma_now / half_width)
    for step_index in range(ORDER - 1):
        sigma_next = 1.0 / (tau_value - sigma_now)
        upcoming = (hamiltonian_fn(current) - centre * current) * (2.0 * sigma_next / half_width) - sigma_now * sigma_next * previous
        previous = current
        current = upcoming
        sigma_now = sigma_next
    return current

def reference(orbitals, potential, projectors, atom_kind, atom_plane, atom_coef, filter_cut, filter_top):
    plane_ids = jnp.arange(GX).astype(jnp.int32)
    depth_ids = jnp.arange(BP).astype(jnp.int32)
    selector = (plane_ids[None, None, :] == atom_plane.astype(jnp.int32)[:, None, None] + depth_ids[None, :, None]).astype(jnp.float32)
    atom_tables = projectors[atom_kind]
    cut_value = filter_cut[0]
    top_value = filter_top[0]

    def hamiltonian_fn(source):
        return hamiltonian(source, potential, selector, atom_tables, atom_coef)
    group_size = 32 if NB % 32 == 0 else NB
    groups = orbitals.reshape(NB // group_size, group_size, GX, GY * GZ)
    filtered = lax.map(lambda group_block: chebyshev(group_block, hamiltonian_fn, cut_value, top_value), groups)
    filtered = filtered.reshape(NB, NPTS)
    gram_matrix = jnp.dot(filtered, filtered.T, precision=highest) / NPTS
    factor = jnp.linalg.cholesky(gram_matrix)
    return jax.scipy.linalg.solve_triangular(factor, filtered, lower=True)
```

```python
import functools

import jax
import jax.numpy as jnp
from jax import lax
from jax.experimental import pallas as pl
from jax.experimental.pallas import tpu as pltpu
from jax.sharding import PartitionSpec as P

GZ = 32
ORDER = 6

low_edge = -1.0
highest = lax.Precision.HIGHEST
f32 = jnp.float32
bf16 = jnp.bfloat16


def transverse_matrix(points, width_z):
    r = jnp.arange(points)
    y, z = r // width_z, r % width_z
    dy = jnp.abs(y[:, None] - y[None, :])
    dz = jnp.abs(z[:, None] - z[None, :])
    line = lambda d: jnp.where(d == 0, -30.0, jnp.where(d == 1, 16.0, jnp.where(d == 2, -1.0, 0.0)))
    return (jnp.where(dz == 0, line(dy), 0.0) + jnp.where(dy == 0, line(dz), 0.0)).astype(bf16)


def filter_kernel(
    plane_ref, kind_ref, scal_ref, orb_ref, pot_ref, coef_ref, lap_ref, proj_ref,
    out_ref, ph_ref, pl_ref, buf, split, trans, spread, halo, send_sem, recv_sem,
):
    planes, rows, points = orb_ref.shape
    atoms = coef_ref.shape[0]
    depth = proj_ref.shape[1]
    size = lax.axis_size("slab")
    me = lax.axis_index("slab")
    right, left = lax.rem(me + 1, size), lax.rem(me + size - 1, size)

    barrier = pltpu.get_barrier_semaphore()
    for neighbour in (left, right):
        pl.semaphore_signal(barrier, inc=1, device_id={"slab": neighbour}, device_id_type=pl.DeviceIdType.MESH)
    pl.semaphore_wait(barrier, 2)

    buf[0] = orb_ref[...]
    buf[1] = jnp.zeros((planes, rows, points), f32)
    for a in range(atoms):
        spread[a, 0] = jnp.zeros((rows, points), f32)
        spread[a, depth + 1] = jnp.zeros((rows, points), f32)
    for k in range(proj_ref.shape[0]):
        for j in range(depth):
            table = proj_ref[k, j]
            high = table.astype(bf16)
            ph_ref[k, j] = high
            pl_ref[k, j] = (table - high.astype(f32)).astype(bf16)
    centre = scal_ref[2 * ORDER]

    def step(s, carry):
        cur = lax.rem(s, 2)
        nxt = 1 - cur
        scale = scal_ref[2 * s]
        back = scal_ref[2 * s + 1]
        copies = []
        for side, first, target in ((0, planes - 2, right), (1, 0, left)):
            copy = pltpu.make_async_remote_copy(
                src_ref=buf.at[cur, pl.ds(first, 2)],
                dst_ref=halo.at[s, side],
                send_sem=send_sem.at[side],
                recv_sem=recv_sem.at[s, side],
                device_id={"slab": target},
                device_id_type=pl.DeviceIdType.MESH,
            )
            copy.start()
            copies.append(copy)

        group = 4 if planes % 4 == 0 else 1

        def lap_group(g, c):
            x0 = g * group
            f = buf[cur, pl.ds(x0, group)]
            hi = f.astype(bf16)
            lo = (f - hi.astype(f32)).astype(bf16)
            both = jnp.concatenate([hi, lo], axis=1)
            split[pl.ds(x0, group)] = both
            r = jnp.dot(both.reshape(group * 2 * rows, points), lap_ref[...], preferred_element_type=f32)
            r = r.reshape(group, 2 * rows, points)
            trans[pl.ds(x0, group)] = r[:, :rows] + r[:, rows:]
            return c

        lax.fori_loop(0, planes // group, lap_group, 0)

        def atom(a, c):
            p = plane_ref[a]
            k = kind_ref[a]
            coupled = jnp.zeros((rows, ph_ref.shape[3]), f32)
            for j in range(depth):
                both = split[p + j]
                r = jnp.dot(both, ph_ref[k, j], preferred_element_type=f32)
                e = jnp.dot(both[:rows], pl_ref[k, j], preferred_element_type=f32)
                coupled = coupled + (r[:rows] + (r[rows:] + e))
            coupled = coupled * coef_ref[a]
            hi = coupled.astype(bf16)
            lo = (coupled - hi.astype(f32)).astype(bf16)
            both = jnp.concatenate([hi, lo], axis=0)
            nt = (((1,), (1,)), ((), ()))
            for j in range(depth):
                r = lax.dot_general(both, ph_ref[k, j], nt, preferred_element_type=f32)
                e = lax.dot_general(hi, pl_ref[k, j], nt, preferred_element_type=f32)
                spread[a, j + 1] = r[:rows] + (r[rows:] + e)
            return c

        lax.fori_loop(0, atoms, atom, 0)

        piece = 16 if rows % 16 == 0 else 8

        def plane(x, sources):
            slots = [jnp.clip(x - plane_ref[a], -1, depth) + 1 for a in range(atoms)]
            for r0 in range(0, rows, piece):
                rs = pl.ds(r0, piece)
                f = buf[cur, x, rs]
                m2, m1, p1, p2 = [ref[index + (rs,)] for ref, index in sources]
                total = trans[x, rs] * (-0.5 / 12.0) + (pot_ref[x] + (1.25 - centre)) * f
                total = total + (m1 + p1) * (-2.0 / 3.0) + (m2 + p2) * (1.0 / 24.0)
                for a in range(atoms):
                    total = total + spread[a, slots[a], rs]
                buf[nxt, x, rs] = scale * total - back * buf[nxt, x, rs]

        def interior(x, c):
            plane(x, [(buf, (cur, x + d)) for d in (-2, -1, 1, 2)])
            return c

        lax.fori_loop(2, planes - 2, interior, 0)
        for copy in copies:
            copy.wait()

        def source(x):
            if x < 0:
                return halo, (s, 0, x + 2)
            if x >= planes:
                return halo, (s, 1, x - planes)
            return buf, (cur, x)

        for x in (0, 1, planes - 2, planes - 1):
            plane(x, [source(x + d) for d in (-2, -1, 1, 2)])
        return carry

    lax.fori_loop(0, ORDER, step, 0)
    width = out_ref.shape[2]
    unit = min(width, points)
    for start in range(0, planes * points, unit):
        x, at = start // points, start % points
        chunk, lane = start // width, start % width
        out_ref[chunk, :, lane : lane + unit] = buf[ORDER % 2, x, :, at : at + unit]


def filter_call(plane, kind, scal, orb, pot, coef, lap, tables, chunks):
    planes, rows, points = orb.shape
    atoms = coef.shape[0]
    depth = tables.shape[1]
    smem = pl.BlockSpec(memory_space=pltpu.SMEM)
    vmem = pl.BlockSpec(memory_space=pltpu.VMEM)
    return pl.pallas_call(
        filter_kernel,
        out_shape=jax.ShapeDtypeStruct((chunks, rows, planes * points // chunks), f32),
        in_specs=[smem] * 3 + [vmem] * 5,
        out_specs=vmem,
        scratch_shapes=[
            pltpu.VMEM(tables.shape, bf16),
            pltpu.VMEM(tables.shape, bf16),
            pltpu.VMEM((2, planes, rows, points), f32),
            pltpu.VMEM((planes, 2 * rows, points), bf16),
            pltpu.VMEM((planes, rows, points), f32),
            pltpu.VMEM((atoms, depth + 2, rows, points), f32),
            pltpu.VMEM((ORDER, 2, 2, rows, points), f32),
            pltpu.SemaphoreType.DMA((2,)),
            pltpu.SemaphoreType.DMA((ORDER, 2)),
        ],
        compiler_params=pltpu.CompilerParams(
            collective_id=0, has_side_effects=True, vmem_limit_bytes=56 * 1024 * 1024
        ),
        name="cheb_filter",
    )(plane, kind, scal, orb, pot, coef, lap, tables)


def factor_kernel(nb, g_ref, w_ref, a_ref, d_ref):
    n = g_ref.shape[0]
    a_ref[...] = g_ref[...]
    w_ref[...] = jnp.zeros((n, n), f32)
    rows = lax.broadcasted_iota(jnp.int32, (nb, nb), 0)
    cols = lax.broadcasted_iota(jnp.int32, (nb, nb), 1)
    row_ids = lax.broadcasted_iota(jnp.int32, (nb, 1), 0)
    lane_ids = lax.broadcasted_iota(jnp.int32, (1, nb), 1)
    nt = (((1,), (1,)), ((), ()))
    for b in range(n // nb):
        lo, hi = b * nb, (b + 1) * nb
        d_ref[:, :nb] = a_ref[lo:hi, lo:hi]
        d_ref[:, nb:] = (rows == cols).astype(f32)

        def eliminate(k, c):
            row = d_ref[pl.ds(k, 1), :]
            pivot = jnp.sum(jnp.where(lane_ids == k, row[:, :nb], 0.0), axis=1, keepdims=True)
            column = jnp.sum(jnp.where(cols == k, d_ref[:, :nb], 0.0), axis=1, keepdims=True)
            ratio = jnp.where(row_ids > k, column, 0.0)
            d_ref[...] = d_ref[...] - ratio * (row * (1.0 / pivot))
            return c

        lax.fori_loop(0, nb, eliminate, 0)
        pivots = jnp.sum(jnp.where(rows == cols, d_ref[:, :nb], 0.0), axis=1, keepdims=True)
        inverse = d_ref[:, nb:] / jnp.sqrt(pivots)
        w_ref[lo:hi, lo:hi] = inverse
        if lo > 0:
            mixed = jnp.dot(a_ref[lo:hi, :lo], w_ref[:lo, :lo], precision=highest, preferred_element_type=f32)
            w_ref[lo:hi, :lo] = -jnp.dot(inverse, mixed, precision=highest, preferred_element_type=f32)
        if hi < n:
            panel = lax.dot_general(a_ref[hi:, lo:hi], inverse, nt, precision=highest, preferred_element_type=f32)
            a_ref[hi:, lo:hi] = panel
            a_ref[hi:, hi:] = a_ref[hi:, hi:] - lax.dot_general(
                panel, panel, nt, precision=highest, preferred_element_type=f32
            )


def inverse_factor(gram):
    n = gram.shape[0]
    nb = 128 if n % 128 == 0 else n
    vmem = pl.BlockSpec(memory_space=pltpu.VMEM)
    return pl.pallas_call(
        functools.partial(factor_kernel, nb),
        out_shape=jax.ShapeDtypeStruct((n, n), f32),
        in_specs=[vmem],
        out_specs=vmem,
        scratch_shapes=[pltpu.VMEM((n, n), f32), pltpu.VMEM((nb, 2 * nb), f32)],
        compiler_params=pltpu.CompilerParams(vmem_limit_bytes=32 * 1024 * 1024),
        name="factor_inverse",
    )(gram)


def reduce_axis(value, axis):
    size = lax.axis_size(axis)
    pieces = value.reshape((size, value.shape[0] // size) + value.shape[1:])
    pieces = lax.all_to_all(pieces, axis, split_axis=0, concat_axis=0, tiled=True)
    return jnp.sum(pieces, axis=0)


def gather_axis(value, axis):
    size = lax.axis_size(axis)
    pieces = jnp.broadcast_to(value[None], (size,) + value.shape)
    pieces = lax.all_to_all(pieces, axis, split_axis=0, concat_axis=0, tiled=True)
    return pieces.reshape((size * value.shape[0],) + value.shape[1:])


def local(
    orbitals, potential, projectors, atom_kind, atom_plane, atom_coef, filter_cut, filter_top
):
    band_count, planes, points = orbitals.shape
    kind_count, block_pts, func_count = projectors.shape
    atom_count = atom_kind.shape[0]
    depth = block_pts // points
    bands = lax.axis_size("band")
    local_plane = (atom_plane - lax.axis_index("slab") * planes).astype(jnp.int32)

    cut_value = filter_cut[0]
    top_value = filter_top[0]
    half_width = (top_value - cut_value) / 2.0
    centre = (top_value + cut_value) / 2.0
    sigma_now = half_width / (low_edge - centre)
    tau_value = 2.0 / sigma_now
    scal = [sigma_now / half_width, jnp.zeros((), f32)]
    for _ in range(ORDER - 1):
        sigma_next = 1.0 / (tau_value - sigma_now)
        scal += [2.0 * sigma_next / half_width, sigma_now * sigma_next]
        sigma_now = sigma_next
    scal = jnp.stack(scal + [centre])

    tables = projectors.reshape(kind_count, depth, points, func_count)
    filtered = filter_call(
        local_plane, atom_kind, scal,
        jnp.transpose(orbitals, (1, 0, 2)), potential.reshape(planes, 1, points),
        atom_coef.reshape(atom_count, 1, func_count), transverse_matrix(points, GZ), tables, bands,
    )
    grid_layout = lax.all_to_all(filtered, "band", split_axis=0, concat_axis=0, tiled=True)
    grid_layout = grid_layout.reshape(bands * band_count, planes * points // bands)
    point_total = grid_layout.shape[1] * lax.axis_size(("band", "slab"))
    gram = jnp.dot(grid_layout, grid_layout.T, precision=highest) / point_total
    gram = reduce_axis(reduce_axis(gram, "slab"), "band")
    gram = gather_axis(gather_axis(gram, "band"), "slab")
    return jnp.dot(inverse_factor(gram), grid_layout, precision=lax.Precision.HIGH)


def solution(mesh):
    in_specs = (
        P("band", "slab", None),
        P("slab", None),
        P(),
        P("slab"),
        P("slab"),
        P("slab", None),
        P(),
        P(),
    )
    out_specs = P(None, ("slab", "band"))
    return jax.shard_map(local, mesh=mesh, in_specs=in_specs, out_specs=out_specs, check_vma=False)
```

```python
import functools

import jax
import jax.numpy as jnp
from jax import lax
from jax.experimental import pallas as pl
from jax.experimental.pallas import tpu as pltpu
from jax.sharding import PartitionSpec as P

GZ = 32
ORDER = 6

low_edge = -1.0
highest = lax.Precision.HIGHEST
f32 = jnp.float32
bf16 = jnp.bfloat16


def transverse_matrix(points, width_z):
    r = jnp.arange(points)
    y, z = r // width_z, r % width_z
    dy = jnp.abs(y[:, None] - y[None, :])
    dz = jnp.abs(z[:, None] - z[None, :])
    line = lambda d: jnp.where(d == 0, -30.0, jnp.where(d == 1, 16.0, jnp.where(d == 2, -1.0, 0.0)))
    return (jnp.where(dz == 0, line(dy), 0.0) + jnp.where(dy == 0, line(dz), 0.0)).astype(bf16)


def filter_kernel(
    plane_ref, kind_ref, scal_ref, orb_ref, pot_ref, coef_ref, lap_ref, proj_ref,
    out_ref, ph_ref, pl_ref, buf, split, trans, spread, halo, send_sem, recv_sem,
):
    planes, rows, points = orb_ref.shape
    atoms = coef_ref.shape[0]
    depth = proj_ref.shape[1]
    size = lax.axis_size("slab")
    me = lax.axis_index("slab")
    right, left = lax.rem(me + 1, size), lax.rem(me + size - 1, size)

    barrier = pltpu.get_barrier_semaphore()
    for neighbour in (left, right):
        pl.semaphore_signal(barrier, inc=1, device_id={"slab": neighbour}, device_id_type=pl.DeviceIdType.MESH)
    pl.semaphore_wait(barrier, 2)

    buf[0] = orb_ref[...]
    buf[1] = jnp.zeros((planes, rows, points), f32)
    for a in range(atoms):
        spread[a, 0] = jnp.zeros((rows, points), f32)
        spread[a, depth + 1] = jnp.zeros((rows, points), f32)
    for k in range(proj_ref.shape[0]):
        for j in range(depth):
            table = proj_ref[k, j]
            high = table.astype(bf16)
            ph_ref[k, j] = high
            pl_ref[k, j] = (table - high.astype(f32)).astype(bf16)
    centre = scal_ref[2 * ORDER]

    def step(s, carry):
        cur = lax.rem(s, 2)
        nxt = 1 - cur
        scale = scal_ref[2 * s]
        back = scal_ref[2 * s + 1]
        copies = []
        for side, first, target in ((0, planes - 2, right), (1, 0, left)):
            copy = pltpu.make_async_remote_copy(
                src_ref=buf.at[cur, pl.ds(first, 2)],
                dst_ref=halo.at[s, side],
                send_sem=send_sem.at[side],
                recv_sem=recv_sem.at[s, side],
                device_id={"slab": target},
                device_id_type=pl.DeviceIdType.MESH,
            )
            copy.start()
            copies.append(copy)

        group = 4 if planes % 4 == 0 else 1

        def lap_group(g, c):
            x0 = g * group
            f = buf[cur, pl.ds(x0, group)]
            hi = f.astype(bf16)
            lo = (f - hi.astype(f32)).astype(bf16)
            both = jnp.concatenate([hi, lo], axis=1)
            split[pl.ds(x0, group)] = both
            r = jnp.dot(both.reshape(group * 2 * rows, points), lap_ref[...], preferred_element_type=f32)
            r = r.reshape(group, 2 * rows, points)
            trans[pl.ds(x0, group)] = r[:, :rows] + r[:, rows:]
            return c

        lax.fori_loop(0, planes // group, lap_group, 0)

        def atom(a, c):
            p = plane_ref[a]
            k = kind_ref[a]
            coupled = jnp.zeros((rows, ph_ref.shape[3]), f32)
            for j in range(depth):
                both = split[p + j]
                r = jnp.dot(both, ph_ref[k, j], preferred_element_type=f32)
                e = jnp.dot(both[:rows], pl_ref[k, j], preferred_element_type=f32)
                coupled = coupled + (r[:rows] + (r[rows:] + e))
            coupled = coupled * coef_ref[a]
            hi = coupled.astype(bf16)
            lo = (coupled - hi.astype(f32)).astype(bf16)
            both = jnp.concatenate([hi, lo], axis=0)
            nt = (((1,), (1,)), ((), ()))
            for j in range(depth):
                r = lax.dot_general(both, ph_ref[k, j], nt, preferred_element_type=f32)
                e = lax.dot_general(hi, pl_ref[k, j], nt, preferred_element_type=f32)
                spread[a, j + 1] = r[:rows] + (r[rows:] + e)
            return c

        lax.fori_loop(0, atoms, atom, 0)

        piece = 16 if rows % 16 == 0 else 8

        def plane(x, sources):
            slots = [jnp.clip(x - plane_ref[a], -1, depth) + 1 for a in range(atoms)]
            for r0 in range(0, rows, piece):
                rs = pl.ds(r0, piece)
                f = buf[cur, x, rs]
                m2, m1, p1, p2 = [ref[index + (rs,)] for ref, index in sources]
                total = trans[x, rs] * (-0.5 / 12.0) + (pot_ref[x] + (1.25 - centre)) * f
                total = total + (m1 + p1) * (-2.0 / 3.0) + (m2 + p2) * (1.0 / 24.0)
                for a in range(atoms):
                    total = total + spread[a, slots[a], rs]
                buf[nxt, x, rs] = scale * total - back * buf[nxt, x, rs]

        def interior(x, c):
            plane(x, [(buf, (cur, x + d)) for d in (-2, -1, 1, 2)])
            return c

        lax.fori_loop(2, planes - 2, interior, 0)
        for copy in copies:
            copy.wait()

        def source(x):
            if x < 0:
                return halo, (s, 0, x + 2)
            if x >= planes:
                return halo, (s, 1, x - planes)
            return buf, (cur, x)

        for x in (0, 1, planes - 2, planes - 1):
            plane(x, [source(x + d) for d in (-2, -1, 1, 2)])
        return carry

    lax.fori_loop(0, ORDER, step, 0)
    width = out_ref.shape[2]
    unit = min(width, points)
    for start in range(0, planes * points, unit):
        x, at = start // points, start % points
        chunk, lane = start // width, start % width
        out_ref[chunk, :, lane : lane + unit] = buf[ORDER % 2, x, :, at : at + unit]


def filter_call(plane, kind, scal, orb, pot, coef, lap, tables, chunks):
    planes, rows, points = orb.shape
    atoms = coef.shape[0]
    depth = tables.shape[1]
    smem = pl.BlockSpec(memory_space=pltpu.SMEM)
    vmem = pl.BlockSpec(memory_space=pltpu.VMEM)
    return pl.pallas_call(
        filter_kernel,
        out_shape=jax.ShapeDtypeStruct((chunks, rows, planes * points // chunks), f32),
        in_specs=[smem] * 3 + [vmem] * 5,
        out_specs=vmem,
        scratch_shapes=[
            pltpu.VMEM(tables.shape, bf16),
            pltpu.VMEM(tables.shape, bf16),
            pltpu.VMEM((2, planes, rows, points), f32),
            pltpu.VMEM((planes, 2 * rows, points), bf16),
            pltpu.VMEM((planes, rows, points), f32),
            pltpu.VMEM((atoms, depth + 2, rows, points), f32),
            pltpu.VMEM((ORDER, 2, 2, rows, points), f32),
            pltpu.SemaphoreType.DMA((2,)),
            pltpu.SemaphoreType.DMA((ORDER, 2)),
        ],
        compiler_params=pltpu.CompilerParams(
            collective_id=0, has_side_effects=True, vmem_limit_bytes=56 * 1024 * 1024
        ),
        name="cheb_filter",
    )(plane, kind, scal, orb, pot, coef, lap, tables)


def factor_kernel(nb, g_ref, w_ref, a_ref, d_ref):
    n = w_ref.shape[0]
    a_ref[...] = jnp.zeros((n, n), f32)
    at = 0
    for i in range(n // nb):
        for j in range(i + 1):
            a_ref[i * nb : (i + 1) * nb, j * nb : (j + 1) * nb] = g_ref[at : at + nb]
            at += nb
    w_ref[...] = jnp.zeros((n, n), f32)
    rows = lax.broadcasted_iota(jnp.int32, (nb, nb), 0)
    cols = lax.broadcasted_iota(jnp.int32, (nb, nb), 1)
    row_ids = lax.broadcasted_iota(jnp.int32, (nb, 1), 0)
    lane_ids = lax.broadcasted_iota(jnp.int32, (1, nb), 1)
    nt = (((1,), (1,)), ((), ()))
    for b in range(n // nb):
        lo, hi = b * nb, (b + 1) * nb
        d_ref[:, :nb] = a_ref[lo:hi, lo:hi]
        d_ref[:, nb:] = (rows == cols).astype(f32)

        def eliminate(k, c):
            row = d_ref[pl.ds(k, 1), :]
            pivot = jnp.sum(jnp.where(lane_ids == k, row[:, :nb], 0.0), axis=1, keepdims=True)
            column = jnp.sum(jnp.where(cols == k, d_ref[:, :nb], 0.0), axis=1, keepdims=True)
            ratio = jnp.where(row_ids > k, column, 0.0)
            d_ref[...] = d_ref[...] - ratio * (row * (1.0 / pivot))
            return c

        lax.fori_loop(0, nb, eliminate, 0)
        pivots = jnp.sum(jnp.where(rows == cols, d_ref[:, :nb], 0.0), axis=1, keepdims=True)
        inverse = d_ref[:, nb:] / jnp.sqrt(pivots)
        w_ref[lo:hi, lo:hi] = inverse
        if lo > 0:
            mixed = jnp.dot(a_ref[lo:hi, :lo], w_ref[:lo, :lo], precision=highest, preferred_element_type=f32)
            w_ref[lo:hi, :lo] = -jnp.dot(inverse, mixed, precision=highest, preferred_element_type=f32)
        if hi < n:
            panel = lax.dot_general(a_ref[hi:, lo:hi], inverse, nt, precision=highest, preferred_element_type=f32)
            a_ref[hi:, lo:hi] = panel
            a_ref[hi:, hi:] = a_ref[hi:, hi:] - lax.dot_general(
                panel, panel, nt, precision=highest, preferred_element_type=f32
            )


def inverse_factor(blocks, n):
    nb = block_size(n)
    vmem = pl.BlockSpec(memory_space=pltpu.VMEM)
    return pl.pallas_call(
        functools.partial(factor_kernel, nb),
        out_shape=jax.ShapeDtypeStruct((n, n), f32),
        in_specs=[vmem],
        out_specs=vmem,
        scratch_shapes=[pltpu.VMEM((n, n), f32), pltpu.VMEM((nb, 2 * nb), f32)],
        compiler_params=pltpu.CompilerParams(vmem_limit_bytes=32 * 1024 * 1024),
        name="factor_inverse",
    )(blocks)


def reduce_kernel(nb, g_ref, out_ref, pack, first, part, second, full, sends, recvs_a, recvs_b, recvs_c, recvs_d):
    n = g_ref.shape[0]
    total = pack.shape[0]
    slabs, bands = lax.axis_size("slab"), lax.axis_size("band")
    my_slab, my_band = lax.axis_index("slab"), lax.axis_index("band")
    deep, thin = total // slabs, total // slabs // bands
    at = 0
    for i in range(n // nb):
        for j in range(i + 1):
            pack[at : at + nb] = g_ref[i * nb : (i + 1) * nb, j * nb : (j + 1) * nb]
            at += nb
    if at < total:
        pack[at:] = jnp.zeros((total - at, nb), f32)

    def peer(me, size, d):
        return lax.rem(me + d, size)

    barrier = pltpu.get_barrier_semaphore()
    for axis, me, size in (("slab", my_slab, slabs), ("band", my_band, bands)):
        for d in range(1, size):
            pl.semaphore_signal(
                barrier, inc=1, device_id={axis: peer(me, size, d)}, device_id_type=pl.DeviceIdType.MESH
            )
    pl.semaphore_wait(barrier, slabs + bands - 2)

    def exchange(axis, me, size, source, target, recvs):
        copies = []
        for d in range(1, size):
            other = peer(me, size, d)
            copies.append(
                pltpu.make_async_remote_copy(
                    src_ref=source(other),
                    dst_ref=target(d),
                    send_sem=sends.at[d - 1],
                    recv_sem=recvs.at[d - 1],
                    device_id={axis: other},
                    device_id_type=pl.DeviceIdType.MESH,
                )
            )
        for copy in copies:
            copy.start()
        for copy in copies:
            copy.wait()

    def span(start, length):
        return pl.ds(pl.multiple_of(start, 8), length)

    exchange(
        "slab", my_slab, slabs, lambda t: pack.at[span(t * deep, deep)], lambda d: first.at[d - 1], recvs_a
    )
    value = pack[span(my_slab * deep, deep)]
    for d in range(1, slabs):
        value = value + first[d - 1]
    part[...] = value
    exchange(
        "band", my_band, bands, lambda t: part.at[span(t * thin, thin)], lambda d: second.at[d - 1], recvs_b
    )
    value = part[span(my_band * thin, thin)]
    for d in range(1, bands):
        value = value + second[d - 1]
    mine = span(my_slab * deep + my_band * thin, thin)
    full[mine] = value
    exchange("band", my_band, bands, lambda t: full.at[mine], lambda d: full.at[mine], recvs_c)
    mine_deep = span(my_slab * deep, deep)
    exchange("slab", my_slab, slabs, lambda t: full.at[mine_deep], lambda d: full.at[mine_deep], recvs_d)
    out_ref[...] = full[...]


def block_size(n):
    return 128 if n % 128 == 0 else n


def reduced_blocks(gram):
    n = gram.shape[0]
    nb = block_size(n)
    slabs, bands = lax.axis_size("slab"), lax.axis_size("band")
    count = n // nb
    used = count * (count + 1) // 2 * nb
    unit = 8 * slabs * bands
    total = (used + unit - 1) // unit * unit
    vmem = pl.BlockSpec(memory_space=pltpu.VMEM)
    dma = pltpu.SemaphoreType.DMA
    return pl.pallas_call(
        functools.partial(reduce_kernel, nb),
        out_shape=jax.ShapeDtypeStruct((total, nb), f32),
        in_specs=[vmem],
        out_specs=vmem,
        scratch_shapes=[
            pltpu.VMEM((total, nb), f32),
            pltpu.VMEM((slabs - 1, total // slabs, nb), f32),
            pltpu.VMEM((total // slabs, nb), f32),
            pltpu.VMEM((bands - 1, total // slabs // bands, nb), f32),
            pltpu.VMEM((total, nb), f32),
            dma((max(slabs, bands) - 1,)),
            dma((slabs - 1,)),
            dma((bands - 1,)),
            dma((bands - 1,)),
            dma((slabs - 1,)),
        ],
        compiler_params=pltpu.CompilerParams(
            collective_id=1, has_side_effects=True, vmem_limit_bytes=32 * 1024 * 1024
        ),
        name="gram_sum",
    )(gram)


def local(
    orbitals, potential, projectors, atom_kind, atom_plane, atom_coef, filter_cut, filter_top
):
    band_count, planes, points = orbitals.shape
    kind_count, block_pts, func_count = projectors.shape
    atom_count = atom_kind.shape[0]
    depth = block_pts // points
    bands = lax.axis_size("band")
    local_plane = (atom_plane - lax.axis_index("slab") * planes).astype(jnp.int32)

    cut_value = filter_cut[0]
    top_value = filter_top[0]
    half_width = (top_value - cut_value) / 2.0
    centre = (top_value + cut_value) / 2.0
    sigma_now = half_width / (low_edge - centre)
    tau_value = 2.0 / sigma_now
    scal = [sigma_now / half_width, jnp.zeros((), f32)]
    for _ in range(ORDER - 1):
        sigma_next = 1.0 / (tau_value - sigma_now)
        scal += [2.0 * sigma_next / half_width, sigma_now * sigma_next]
        sigma_now = sigma_next
    scal = jnp.stack(scal + [centre])

    tables = projectors.reshape(kind_count, depth, points, func_count)
    filtered = filter_call(
        local_plane, atom_kind, scal,
        jnp.transpose(orbitals, (1, 0, 2)), potential.reshape(planes, 1, points),
        atom_coef.reshape(atom_count, 1, func_count), transverse_matrix(points, GZ), tables, bands,
    )
    grid_layout = lax.all_to_all(filtered, "band", split_axis=0, concat_axis=0, tiled=True)
    grid_layout = grid_layout.reshape(bands * band_count, planes * points // bands)
    point_total = grid_layout.shape[1] * lax.axis_size(("band", "slab"))
    gram = jnp.dot(grid_layout, grid_layout.T, precision=highest) / point_total
    factor_inverse = inverse_factor(reduced_blocks(gram), gram.shape[0])
    return jnp.dot(factor_inverse, grid_layout, precision=lax.Precision.HIGH)


def solution(mesh):
    in_specs = (
        P("band", "slab", None),
        P("slab", None),
        P(),
        P("slab"),
        P("slab"),
        P("slab", None),
        P(),
        P(),
    )
    out_specs = P(None, ("slab", "band"))
    return jax.shard_map(local, mesh=mesh, in_specs=in_specs, out_specs=out_specs, check_vma=False)
```

```python
import functools

import jax
import jax.numpy as jnp
from jax import lax
from jax.experimental import pallas as pl
from jax.experimental.pallas import tpu as pltpu
from jax.sharding import PartitionSpec as P

GZ = 32
ORDER = 6

low_edge = -1.0
highest = lax.Precision.HIGHEST
f32 = jnp.float32
bf16 = jnp.bfloat16


def transverse_matrix(points, width_z):
    r = jnp.arange(points)
    y, z = r // width_z, r % width_z
    dy = jnp.abs(y[:, None] - y[None, :])
    dz = jnp.abs(z[:, None] - z[None, :])
    line = lambda d: jnp.where(d == 0, -30.0, jnp.where(d == 1, 16.0, jnp.where(d == 2, -1.0, 0.0)))
    return (jnp.where(dz == 0, line(dy), 0.0) + jnp.where(dy == 0, line(dz), 0.0)).astype(bf16)


def filter_kernel(
    plane_ref, kind_ref, scal_ref, orb_ref, pot_ref, coef_ref, lap_ref, proj_ref,
    out_ref, ph_ref, pl_ref, buf, split, trans, spread, halo, send_sem, recv_sem,
):
    planes, rows, points = orb_ref.shape
    atoms = coef_ref.shape[0]
    depth = proj_ref.shape[1]
    size = lax.axis_size("slab")
    me = lax.axis_index("slab")
    right, left = lax.rem(me + 1, size), lax.rem(me + size - 1, size)

    barrier = pltpu.get_barrier_semaphore()
    for neighbour in (left, right):
        pl.semaphore_signal(barrier, inc=1, device_id={"slab": neighbour}, device_id_type=pl.DeviceIdType.MESH)
    pl.semaphore_wait(barrier, 2)

    buf[0] = orb_ref[...]
    buf[1] = jnp.zeros((planes, rows, points), f32)
    for a in range(atoms):
        spread[a, 0] = jnp.zeros((rows, points), f32)
        spread[a, depth + 1] = jnp.zeros((rows, points), f32)
    for k in range(proj_ref.shape[0]):
        for j in range(depth):
            table = proj_ref[k, j]
            high = table.astype(bf16)
            ph_ref[k, j] = high
            pl_ref[k, j] = (table - high.astype(f32)).astype(bf16)
    centre = scal_ref[2 * ORDER]

    def step(s, carry):
        cur = lax.rem(s, 2)
        nxt = 1 - cur
        scale = scal_ref[2 * s]
        back = scal_ref[2 * s + 1]
        copies = []
        for side, first, target in ((0, planes - 2, right), (1, 0, left)):
            copy = pltpu.make_async_remote_copy(
                src_ref=buf.at[cur, pl.ds(first, 2)],
                dst_ref=halo.at[s, side],
                send_sem=send_sem.at[side],
                recv_sem=recv_sem.at[s, side],
                device_id={"slab": target},
                device_id_type=pl.DeviceIdType.MESH,
            )
            copy.start()
            copies.append(copy)

        group = 4 if planes % 4 == 0 else 1

        def lap_group(g, c):
            x0 = g * group
            f = buf[cur, pl.ds(x0, group)]
            hi = f.astype(bf16)
            lo = (f - hi.astype(f32)).astype(bf16)
            both = jnp.concatenate([hi, lo], axis=1)
            split[pl.ds(x0, group)] = both
            r = jnp.dot(both.reshape(group * 2 * rows, points), lap_ref[...], preferred_element_type=f32)
            r = r.reshape(group, 2 * rows, points)
            trans[pl.ds(x0, group)] = r[:, :rows] + r[:, rows:]
            return c

        lax.fori_loop(0, planes // group, lap_group, 0)

        def atom(a, c):
            p = plane_ref[a]
            k = kind_ref[a]
            coupled = jnp.zeros((rows, ph_ref.shape[3]), f32)
            for j in range(depth):
                both = split[p + j]
                r = jnp.dot(both, ph_ref[k, j], preferred_element_type=f32)
                e = jnp.dot(both[:rows], pl_ref[k, j], preferred_element_type=f32)
                coupled = coupled + (r[:rows] + (r[rows:] + e))
            coupled = coupled * coef_ref[a]
            hi = coupled.astype(bf16)
            lo = (coupled - hi.astype(f32)).astype(bf16)
            both = jnp.concatenate([hi, lo], axis=0)
            nt = (((1,), (1,)), ((), ()))
            for j in range(depth):
                r = lax.dot_general(both, ph_ref[k, j], nt, preferred_element_type=f32)
                e = lax.dot_general(hi, pl_ref[k, j], nt, preferred_element_type=f32)
                spread[a, j + 1] = r[:rows] + (r[rows:] + e)
            return c

        lax.fori_loop(0, atoms, atom, 0)

        piece = 16 if rows % 16 == 0 else 8

        def plane(x, sources):
            slots = [jnp.clip(x - plane_ref[a], -1, depth) + 1 for a in range(atoms)]
            for r0 in range(0, rows, piece):
                rs = pl.ds(r0, piece)
                f = buf[cur, x, rs]
                m2, m1, p1, p2 = [ref[index + (rs,)] for ref, index in sources]
                total = trans[x, rs] * (-0.5 / 12.0) + (pot_ref[x] + (1.25 - centre)) * f
                total = total + (m1 + p1) * (-2.0 / 3.0) + (m2 + p2) * (1.0 / 24.0)
                for a in range(atoms):
                    total = total + spread[a, slots[a], rs]
                buf[nxt, x, rs] = scale * total - back * buf[nxt, x, rs]

        def interior(x, c):
            plane(x, [(buf, (cur, x + d)) for d in (-2, -1, 1, 2)])
            return c

        lax.fori_loop(2, planes - 2, interior, 0)
        for copy in copies:
            copy.wait()

        def source(x):
            if x < 0:
                return halo, (s, 0, x + 2)
            if x >= planes:
                return halo, (s, 1, x - planes)
            return buf, (cur, x)

        for x in (0, 1, planes - 2, planes - 1):
            plane(x, [source(x + d) for d in (-2, -1, 1, 2)])
        return carry

    lax.fori_loop(0, ORDER, step, 0)
    width = out_ref.shape[2]
    unit = min(width, points)
    for start in range(0, planes * points, unit):
        x, at = start // points, start % points
        chunk, lane = start // width, start % width
        out_ref[chunk, :, lane : lane + unit] = buf[ORDER % 2, x, :, at : at + unit]


def filter_call(plane, kind, scal, orb, pot, coef, lap, tables, chunks):
    planes, rows, points = orb.shape
    atoms = coef.shape[0]
    depth = tables.shape[1]
    smem = pl.BlockSpec(memory_space=pltpu.SMEM)
    vmem = pl.BlockSpec(memory_space=pltpu.VMEM)
    return pl.pallas_call(
        filter_kernel,
        out_shape=jax.ShapeDtypeStruct((chunks, rows, planes * points // chunks), f32),
        in_specs=[smem] * 3 + [vmem] * 5,
        out_specs=vmem,
        scratch_shapes=[
            pltpu.VMEM(tables.shape, bf16),
            pltpu.VMEM(tables.shape, bf16),
            pltpu.VMEM((2, planes, rows, points), f32),
            pltpu.VMEM((planes, 2 * rows, points), bf16),
            pltpu.VMEM((planes, rows, points), f32),
            pltpu.VMEM((atoms, depth + 2, rows, points), f32),
            pltpu.VMEM((ORDER, 2, 2, rows, points), f32),
            pltpu.SemaphoreType.DMA((2,)),
            pltpu.SemaphoreType.DMA((ORDER, 2)),
        ],
        compiler_params=pltpu.CompilerParams(
            collective_id=0, has_side_effects=True, vmem_limit_bytes=56 * 1024 * 1024
        ),
        name="cheb_filter",
    )(plane, kind, scal, orb, pot, coef, lap, tables)


def factor_kernel(nb, g_ref, w_ref, a_ref, d_ref):
    n = w_ref.shape[0]
    a_ref[...] = jnp.zeros((n, n), f32)
    at = 0
    for i in range(n // nb):
        for j in range(i + 1):
            a_ref[i * nb : (i + 1) * nb, j * nb : (j + 1) * nb] = g_ref[at : at + nb]
            at += nb
    w_ref[...] = jnp.zeros((n, n), f32)
    rows = lax.broadcasted_iota(jnp.int32, (nb, nb), 0)
    cols = lax.broadcasted_iota(jnp.int32, (nb, nb), 1)
    row_ids = lax.broadcasted_iota(jnp.int32, (nb, 1), 0)
    lane_ids = lax.broadcasted_iota(jnp.int32, (1, nb), 1)
    nt = (((1,), (1,)), ((), ()))
    for b in range(n // nb):
        lo, hi = b * nb, (b + 1) * nb
        d_ref[:, :nb] = a_ref[lo:hi, lo:hi]
        d_ref[:, nb:] = (rows == cols).astype(f32)

        def eliminate(t, c):
            k = 2 * t
            top = d_ref[pl.ds(k, 1), :]
            low = d_ref[pl.ds(k + 1, 1), :]
            block = d_ref[:, :nb]

            def lane(row, at):
                return jnp.sum(jnp.where(lane_ids == at, row[:, :nb], 0.0), axis=1, keepdims=True)

            def column(at):
                return jnp.sum(jnp.where(cols == at, block, 0.0), axis=1, keepdims=True)

            p11, p12, p22 = lane(top, k), lane(top, k + 1), lane(low, k + 1)
            c0, c1 = column(k), column(k + 1)
            inv1 = 1.0 / p11
            link = p12 * inv1
            inv2 = 1.0 / (p22 - p12 * link)
            low = (low - link * top) * inv2
            c1 = jnp.where(row_ids > k + 1, c1 - link * c0, 0.0)
            c0 = jnp.where(row_ids > k, c0, 0.0)
            d_ref[...] = d_ref[...] - c0 * (top * inv1) - c1 * low
            return c

        lax.fori_loop(0, nb // 2, eliminate, 0)
        pivots = jnp.sum(jnp.where(rows == cols, d_ref[:, :nb], 0.0), axis=1, keepdims=True)
        inverse = d_ref[:, nb:] / jnp.sqrt(pivots)
        w_ref[lo:hi, lo:hi] = inverse
        if lo > 0:
            mixed = jnp.dot(a_ref[lo:hi, :lo], w_ref[:lo, :lo], precision=highest, preferred_element_type=f32)
            w_ref[lo:hi, :lo] = -jnp.dot(inverse, mixed, precision=highest, preferred_element_type=f32)
        if hi < n:
            panel = lax.dot_general(a_ref[hi:, lo:hi], inverse, nt, precision=highest, preferred_element_type=f32)
            a_ref[hi:, lo:hi] = panel
            a_ref[hi:, hi:] = a_ref[hi:, hi:] - lax.dot_general(
                panel, panel, nt, precision=highest, preferred_element_type=f32
            )


def inverse_factor(blocks, n):
    nb = block_size(n)
    vmem = pl.BlockSpec(memory_space=pltpu.VMEM)
    return pl.pallas_call(
        functools.partial(factor_kernel, nb),
        out_shape=jax.ShapeDtypeStruct((n, n), f32),
        in_specs=[vmem],
        out_specs=vmem,
        scratch_shapes=[pltpu.VMEM((n, n), f32), pltpu.VMEM((nb, 2 * nb), f32)],
        compiler_params=pltpu.CompilerParams(vmem_limit_bytes=32 * 1024 * 1024),
        name="factor_inverse",
    )(blocks)


def reduce_kernel(nb, g_ref, out_ref, pack, first, part, second, full, sends, recvs_a, recvs_b, recvs_c, recvs_d):
    n = g_ref.shape[0]
    total = pack.shape[0]
    slabs, bands = lax.axis_size("slab"), lax.axis_size("band")
    my_slab, my_band = lax.axis_index("slab"), lax.axis_index("band")
    deep, thin = total // slabs, total // slabs // bands
    at = 0
    for i in range(n // nb):
        for j in range(i + 1):
            pack[at : at + nb] = g_ref[i * nb : (i + 1) * nb, j * nb : (j + 1) * nb]
            at += nb
    if at < total:
        pack[at:] = jnp.zeros((total - at, nb), f32)

    def peer(me, size, d):
        return lax.rem(me + d, size)

    barrier = pltpu.get_barrier_semaphore()
    for axis, me, size in (("slab", my_slab, slabs), ("band", my_band, bands)):
        for d in range(1, size):
            pl.semaphore_signal(
                barrier, inc=1, device_id={axis: peer(me, size, d)}, device_id_type=pl.DeviceIdType.MESH
            )
    pl.semaphore_wait(barrier, slabs + bands - 2)

    def exchange(axis, me, size, source, target, recvs):
        copies = []
        for d in range(1, size):
            other = peer(me, size, d)
            copies.append(
                pltpu.make_async_remote_copy(
                    src_ref=source(other),
                    dst_ref=target(d),
                    send_sem=sends.at[d - 1],
                    recv_sem=recvs.at[d - 1],
                    device_id={axis: other},
                    device_id_type=pl.DeviceIdType.MESH,
                )
            )
        for copy in copies:
            copy.start()
        for copy in copies:
            copy.wait()

    def span(start, length):
        return pl.ds(pl.multiple_of(start, 8), length)

    exchange(
        "slab", my_slab, slabs, lambda t: pack.at[span(t * deep, deep)], lambda d: first.at[d - 1], recvs_a
    )
    value = pack[span(my_slab * deep, deep)]
    for d in range(1, slabs):
        value = value + first[d - 1]
    part[...] = value
    exchange(
        "band", my_band, bands, lambda t: part.at[span(t * thin, thin)], lambda d: second.at[d - 1], recvs_b
    )
    value = part[span(my_band * thin, thin)]
    for d in range(1, bands):
        value = value + second[d - 1]
    mine = span(my_slab * deep + my_band * thin, thin)
    full[mine] = value
    exchange("band", my_band, bands, lambda t: full.at[mine], lambda d: full.at[mine], recvs_c)
    mine_deep = span(my_slab * deep, deep)
    exchange("slab", my_slab, slabs, lambda t: full.at[mine_deep], lambda d: full.at[mine_deep], recvs_d)
    out_ref[...] = full[...]


def block_size(n):
    return 128 if n % 128 == 0 else n


def reduced_blocks(gram):
    n = gram.shape[0]
    nb = block_size(n)
    slabs, bands = lax.axis_size("slab"), lax.axis_size("band")
    count = n // nb
    used = count * (count + 1) // 2 * nb
    unit = 8 * slabs * bands
    total = (used + unit - 1) // unit * unit
    vmem = pl.BlockSpec(memory_space=pltpu.VMEM)
    dma = pltpu.SemaphoreType.DMA
    return pl.pallas_call(
        functools.partial(reduce_kernel, nb),
        out_shape=jax.ShapeDtypeStruct((total, nb), f32),
        in_specs=[vmem],
        out_specs=vmem,
        scratch_shapes=[
            pltpu.VMEM((total, nb), f32),
            pltpu.VMEM((slabs - 1, total // slabs, nb), f32),
            pltpu.VMEM((total // slabs, nb), f32),
            pltpu.VMEM((bands - 1, total // slabs // bands, nb), f32),
            pltpu.VMEM((total, nb), f32),
            dma((max(slabs, bands) - 1,)),
            dma((slabs - 1,)),
            dma((bands - 1,)),
            dma((bands - 1,)),
            dma((slabs - 1,)),
        ],
        compiler_params=pltpu.CompilerParams(
            collective_id=1, has_side_effects=True, vmem_limit_bytes=32 * 1024 * 1024
        ),
        name="gram_sum",
    )(gram)


def local(
    orbitals, potential, projectors, atom_kind, atom_plane, atom_coef, filter_cut, filter_top
):
    band_count, planes, points = orbitals.shape
    kind_count, block_pts, func_count = projectors.shape
    atom_count = atom_kind.shape[0]
    depth = block_pts // points
    bands = lax.axis_size("band")
    local_plane = (atom_plane - lax.axis_index("slab") * planes).astype(jnp.int32)

    cut_value = filter_cut[0]
    top_value = filter_top[0]
    half_width = (top_value - cut_value) / 2.0
    centre = (top_value + cut_value) / 2.0
    sigma_now = half_width / (low_edge - centre)
    tau_value = 2.0 / sigma_now
    scal = [sigma_now / half_width, jnp.zeros((), f32)]
    for _ in range(ORDER - 1):
        sigma_next = 1.0 / (tau_value - sigma_now)
        scal += [2.0 * sigma_next / half_width, sigma_now * sigma_next]
        sigma_now = sigma_next
    scal = jnp.stack(scal + [centre])

    tables = projectors.reshape(kind_count, depth, points, func_count)
    filtered = filter_call(
        local_plane, atom_kind, scal,
        jnp.transpose(orbitals, (1, 0, 2)), potential.reshape(planes, 1, points),
        atom_coef.reshape(atom_count, 1, func_count), transverse_matrix(points, GZ), tables, bands,
    )
    grid_layout = lax.all_to_all(filtered, "band", split_axis=0, concat_axis=0, tiled=True)
    grid_layout = grid_layout.reshape(bands * band_count, planes * points // bands)
    point_total = grid_layout.shape[1] * lax.axis_size(("band", "slab"))
    gram = jnp.dot(grid_layout, grid_layout.T, precision=highest) / point_total
    factor_inverse = inverse_factor(reduced_blocks(gram), gram.shape[0])
    return jnp.dot(factor_inverse, grid_layout, precision=lax.Precision.HIGH)


def solution(mesh):
    in_specs = (
        P("band", "slab", None),
        P("slab", None),
        P(),
        P("slab"),
        P("slab"),
        P("slab", None),
        P(),
        P(),
    )
    out_specs = P(None, ("slab", "band"))
    return jax.shard_map(local, mesh=mesh, in_specs=in_specs, out_specs=out_specs, check_vma=False)
```
